32 devices in a mesh: part: 2 (over x), ray: 4 (over z), pix: 4 (over y, core).
Axes of the slice: x: 2, y: 2, z: 4, core: 2. Of those that a mesh axis runs over, the one named last changes fastest.
Arguments:
- sys_mat: bfloat16 [23040, 16384], P('ray', 'pix')
- x_init: float32 [16384, 512], P('pix', 'part'), parts along dimension 1
- sinogram: float32 [23040, 512], P('ray', 'part'), parts along dimension 1
- row_inv: float32 [23040], P('ray')
- col_inv: float32 [16384], P('pix')
- relaxation: float32 [], replicated
Outputs:
- output 1: float32 [16384, 512], P('pix', 'part'), parts along dimension 1
- output 2: float32 [23040, 512], P('ray', 'part'), parts along dimension 1
- output 3: float32 [6, 512], P(None, 'part'), parts along dimension 1
There are 2 independent parts. The reference program is written for one: setup_inputs(seed, part) draws one part's arguments, and reference() takes and returns one part's arrays. A program takes and returns all parts, laid end to end along the dimension named above; an argument that names none is the same for every part.
All inputs are finite; a program needn't handle non-finite values.
Results may differ from the reference program's by a relative error of at most 0.001.
Values are sent between devices in bfloat16 or wider.
A program may use at most 1 GiB of HBM per device.

```python
import jax
import jax.numpy as jnp
from jax import lax

RAYS = 23040
PIXELS = 16384
SLICES = 256
SWEEPS = 6
ROW_BLOCK = 128
FIELD_MODES = 8


def smooth_modes():
    grid_pos = (jnp.arange(PIXELS, dtype=jnp.float32) + 0.5) / PIXELS
    mode_ids = jnp.arange(1, FIELD_MODES + 1, dtype=jnp.float32)
    phase_arg = 2.0 * jnp.pi * grid_pos[:, None] * mode_ids[None, :]
    mode_basis = jnp.concatenate([jnp.cos(phase_arg), jnp.sin(phase_arg)], axis=1)
    return grid_pos, mode_basis, jnp.concatenate([mode_ids, mode_ids])


def draw_image(key_img, mode_basis, mode_ids):
    key_off, key_coef, key_white = jax.random.split(key_img, 3)
    offsets = 0.3 * jax.random.normal(key_off, (SLICES,), jnp.float32)
    mode_coef = jax.random.normal(key_coef, (2 * FIELD_MODES, SLICES), jnp.float32) * (0.5 / jnp.sqrt(mode_ids))[:, None]
    white_noise = 0.1 * jax.random.normal(key_white, (PIXELS, SLICES), jnp.float32)
    smooth_part = jnp.dot(mode_basis, mode_coef, preferred_element_type=jnp.float32)
    return 1.0 + offsets[None, :] + smooth_part + white_noise


def setup_inputs(seed: int = 0, part: int = 0) -> dict:
    base_key = jax.random.key(seed)
    key_mat, key_row, key_col, key_relax = jax.random.split(base_key, 4)
    part_key = jax.random.fold_in(jax.random.key(seed + 1), part)
    key_start, key_truth, key_noise = jax.random.split(part_key, 3)
    grid_pos, mode_basis, mode_ids = smooth_modes()
    x_init = draw_image(key_start, mode_basis, mode_ids)
    x_true = draw_image(key_truth, mode_basis, mode_ids)

    def row_block(col_sum, block_id):
        ray_pos = (block_id.astype(jnp.float32) * ROW_BLOCK + jnp.arange(ROW_BLOCK, dtype=jnp.float32) + 0.5) / RAYS
        scaled_dist = (ray_pos[:, None] - grid_pos[None, :]) / 0.03
        jitter = jax.random.uniform(jax.random.fold_in(key_mat, block_id), (ROW_BLOCK, PIXELS), jnp.float32)
        block_val = ((0.02 + jnp.exp(-scaled_dist * scaled_dist)) * (0.5 + jitter)).astype(jnp.bfloat16)
        block_f32 = block_val.astype(jnp.float32)
        clean_rows = jnp.dot(block_f32, x_true, preferred_element_type=jnp.float32)
        new_sum = col_sum + jnp.sum(block_f32, axis=0)
        return new_sum, (block_val, clean_rows, jnp.sum(block_f32, axis=1))

    col_sum, (blocks, clean_sino, row_sum) = lax.scan(row_block, jnp.zeros((PIXELS,), jnp.float32), jnp.arange(RAYS // ROW_BLOCK))
    sys_mat = blocks.reshape(RAYS, PIXELS)
    row_sum = row_sum.reshape(RAYS)
    sino_noise = jax.random.normal(key_noise, (RAYS, SLICES), jnp.float32)
    sinogram = clean_sino.reshape(RAYS, SLICES) + 0.02 * row_sum[:, None] * sino_noise
    row_inv = jax.random.uniform(key_row, (RAYS,), jnp.float32, minval=0.5, maxval=1.0) / row_sum
    col_inv = jax.random.uniform(key_col, (PIXELS,), jnp.float32, minval=0.5, maxval=1.0) / col_sum
    relaxation = jax.random.uniform(key_relax, (), jnp.float32, minval=0.8, maxval=1.6)
    return {"sys_mat": sys_mat, "x_init": x_init, "sinogram": sinogram, "row_inv": row_inv, "col_inv": col_inv, "relaxation": relaxation}


def reference(sys_mat, x_init, sinogram, row_inv, col_inv, relaxation):
    def one_sweep(state_pair, unused):
        image_cur, prev_resid = state_pair
        projected = jnp.dot(sys_mat, image_cur.astype(jnp.bfloat16), preferred_element_type=jnp.float32)
        residual = row_inv[:, None] * (sinogram - projected)
        sq_norm = jnp.sum(residual * residual, axis=0) / RAYS
        back_proj = jnp.dot(residual.astype(jnp.bfloat16).T, sys_mat, preferred_element_type=jnp.float32).T
        image_cur = image_cur + relaxation * col_inv[:, None] * back_proj
        return (image_cur, residual), sq_norm

    init_state = (x_init, jnp.zeros_like(sinogram))
    (x_final, resid_last), sq_norms = lax.scan(one_sweep, init_state, None, length=SWEEPS)
    return x_final, resid_last, sq_norms
```

```python
import functools

import jax
import jax.numpy as jnp
from jax import lax
from jax.experimental import pallas as pl
from jax.experimental.pallas import tpu as pltpu
from jax.sharding import PartitionSpec as P

SWEEPS = 6
MESH = pl.DeviceIdType.MESH
NR = 9
NP = 16
HP = NP // 2
L1, L2, L3, L4 = 1, 2, 4, 5
RL, AL = 2, 2
FSLOTS = NR + L4
ZSLOTS = HP + 3 * RL + 3 * AL
PERIOD = FSLOTS + ZSLOTS
OFFSET = PERIOD // 2
TOTAL = PERIOD * SWEEPS + OFFSET


def sweep_kernel(a_hbm, xb_hbm, x_hbm, sino, rinv, lamcol, x_out, r_out, sq_out,
                 a_v, pbuf, crecv, yrecv, rt, gbuf, zrecv, xf, xb,
                 a_sem, in_sem, crs_s, crs_r, yrs_s, yrs_r, yag_s, yag_r, cag_s, cag_r,
                 zrs_s, zrs_r, zag_s, zag_r, ry_s, ry_r, rc_s, rc_r, rout_sem, xout_sem):
    part, z, pix = lax.axis_index("part"), lax.axis_index("ray"), lax.axis_index("pix")
    y, core = pix // 2, lax.rem(pix, 2)
    partner = (part, z, y * 2 + (1 - core))
    yneigh = (part, z, (1 - y) * 2 + core)
    zlow = (part, jnp.maximum(z - 1, 0), pix)
    zhigh = (part, jnp.minimum(z + 1, 3), pix)
    rows = a_v.shape[0] // NR
    mine64 = pl.ds(pl.multiple_of(core * 64, 64), 64)
    other64 = pl.ds(pl.multiple_of((1 - core) * 64, 64), 64)
    own32 = pl.ds(pl.multiple_of(core * 64 + y * 32, 32), 32)
    nb32 = pl.ds(pl.multiple_of(core * 64 + (1 - y) * 32, 32), 32)

    def a_copy(i):
        sl = pl.ds(pl.multiple_of(i * rows, rows), rows)
        return pltpu.make_async_copy(a_hbm.at[sl], a_v.at[sl], a_sem.at[i])

    half_off = jnp.where(z >= 2, HP, 0)
    xb_copy = pltpu.make_async_copy(xb_hbm, xb, in_sem.at[0])
    xf_copy = pltpu.make_async_copy(x_hbm.at[:, pl.ds(half_off, HP)], xf, in_sem.at[1])
    xb_copy.start()
    for i in range(NR):
        a_copy(i).start()
    xf_copy.start()

    barrier = pltpu.get_barrier_semaphore()
    pl.semaphore_signal(barrier, inc=1, device_id=partner, device_id_type=MESH)
    pl.semaphore_signal(barrier, inc=1, device_id=yneigh, device_id_type=MESH)

    @pl.when(z > 0)
    def _():
        pl.semaphore_signal(barrier, inc=1, device_id=zlow, device_id_type=MESH)

    @pl.when(z < 3)
    def _():
        pl.semaphore_signal(barrier, inc=1, device_id=zhigh, device_id_type=MESH)

    middle = jnp.logical_and(z > 0, z < 3)

    @pl.when(middle)
    def _():
        pl.semaphore_wait(barrier, 4)

    @pl.when(jnp.logical_not(middle))
    def _():
        pl.semaphore_wait(barrier, 3)

    sq_out[...] = jnp.zeros_like(sq_out)
    xb_copy.wait()
    xf_copy.wait()

    def remote(src, dst, ssem, rsem, dev):
        return pltpu.make_async_remote_copy(
            src_ref=src, dst_ref=dst, send_sem=ssem, recv_sem=rsem, device_id=dev, device_id_type=MESH)

    def core_rs(i):
        return remote(pbuf.at[i, other64], crecv.at[i], crs_s.at[i], crs_r.at[i], partner)

    def y_rs(i):
        return remote(pbuf.at[i, nb32], yrecv.at[i], yrs_s.at[i], yrs_r.at[i], yneigh)

    def y_ag(i, buf):
        return remote(buf.at[i, own32], buf.at[i, own32], yag_s.at[i], yag_r.at[i], yneigh)

    def core_ag(i, buf, which):
        sl = own32 if which == 0 else nb32
        return remote(buf.at[i, sl], buf.at[i, sl], cag_s.at[which, i], cag_r.at[which, i], partner)

    def r_local(h, i):
        return pltpu.make_async_copy(pbuf.at[i, own32], r_out.at[h, i, own32], rout_sem.at[i])

    def r_y(h, i):
        return remote(pbuf.at[i, own32], r_out.at[h, i, own32], ry_s.at[i], ry_r.at[i], yneigh)

    def r_core(h, i, which):
        if which == 0:
            src, dst = pbuf.at[i, own32], r_out.at[h, i, own32]
        else:
            src, dst = r_out.at[h, i, nb32], r_out.at[h, i, nb32]
        return remote(src, dst, rc_s.at[which, i], rc_r.at[which, i], partner)

    def x_local(h, c, j):
        return pltpu.make_async_copy(xf.at[h, c], x_out.at[h, j], xout_sem.at[h, c])

    def on(i, n, body):
        pl.when(jnp.logical_and(i >= 0, i < n))(body)

    def z_rs(h, j, dev):
        return remote(gbuf.at[h, j], zrecv.at[j], zrs_s.at[h, j], zrs_r.at[h, j], dev)

    def z_ag(h, j, buf, dev):
        return remote(buf.at[h, j], buf.at[h, j], zag_s.at[h, j], zag_r.at[h, j], dev)

    def by_kind(last, low, high, body):
        @pl.when(jnp.logical_not(last))
        def _():
            body(low)

        @pl.when(last)
        def _():
            body(high)

    def step1(h, v):
        i = v - L1

        def body():
            copy = core_rs(i)
            copy.wait_recv()
            pbuf[i, mine64] += crecv[i]
            y_rs(i).start()
            copy.wait_send()

        on(i, NR, body)

    def forward(h, k, v):
        i = v

        def body():
            if h == 0:
                @pl.when(k == 0)
                def _():
                    a_copy(i).wait()
            xv = jnp.concatenate([xb[h, j] for j in range(NP)], axis=1)
            av = a_v[pl.ds(pl.multiple_of(i * rows, rows), rows), :]
            pbuf[i] = lax.dot_general(xv, av, (((1,), (1,)), ((), ())), preferred_element_type=jnp.float32)
            core_rs(i).start()

        on(i, NR, body)

    def step2(h, k, v, last):
        i = v - L2

        def body():
            copy = y_rs(i)
            copy.wait_recv()
            resid = rinv[i] * (sino[h, i] - (pbuf[i, own32] + yrecv[i]))
            sqr = resid * resid
            fold = sqr[:, :128]
            for t in range(1, rows // 128):
                fold = fold + sqr[:, t * 128:(t + 1) * 128]
            sq_out[k, pl.ds(h * 32, 32)] += fold

            rt[i, own32] = resid.astype(jnp.bfloat16)
            y_ag(i, rt).start()
            core_ag(i, rt, 0).start()

            @pl.when(last)
            def _():
                pbuf[i, own32] = resid
                r_y(h, i).start()
                r_core(h, i, 0).start()
                r_local(h, i).start()

            copy.wait_send()

        on(i, NR, body)

    def step3(h, v, last):
        i = v - L3

        def body():
            remote(rt.at[i, nb32], rt.at[i, nb32], yag_s.at[i], yag_r.at[i], yneigh).wait_recv()
            core_ag(i, rt, 1).start()

            @pl.when(last)
            def _():
                remote(r_out.at[h, i, nb32], r_out.at[h, i, nb32], ry_s.at[i], ry_r.at[i], yneigh).wait_recv()
                r_core(h, i, 1).start()

        on(i, NR, body)

    def backward(h, v, last):
        i = v - L4

        def body():
            for which in (0, 1):
                core_ag(i, rt, which).wait_recv()
            rv = rt[i]
            sl = pl.ds(pl.multiple_of(i * rows, rows), rows)

            width = gbuf.shape[3]
            for j in range(NP):
                lanes = pl.ds(j * width, width)
                prod = jnp.dot(rv, a_v[sl, lanes], preferred_element_type=jnp.float32)
                gbuf[h, j] = jnp.where(i == 0, prod, gbuf[h, j] + prod)

            y_ag(i, rt).wait_send()
            for which in (0, 1):
                core_ag(i, rt, which).wait_send()

            @pl.when(last)
            def _():
                r_y(h, i).wait_send()
                r_local(h, i).wait()
                for which in (0, 1):
                    r_core(h, i, which).wait_recv()
                    r_core(h, i, which).wait_send()

        on(i, NR, body)

    def z_steps(h, v, last):
        zt = v - FSLOTS
        for direction in (0, 1):
            if direction == 0:
                d, down, up = 3 - z, zlow, zhigh
            else:
                d, down, up = z, zhigh, zlow
            base = direction * HP

            def reduce(d=d, down=down, up=up, base=base):
                c = zt - RL * d
                j = base + c

                @pl.when(d > 0)
                def _():
                    z_rs(h, j, down).wait_recv()
                    gbuf[h, j] += zrecv[j]

                @pl.when(d < 3)
                def _():
                    z_rs(h, j, down).start()

                @pl.when(d == 3)
                def _():
                    new = xf[h, c] + lamcol[j] * gbuf[h, j]

                    @pl.when(jnp.logical_not(last))
                    def _():
                        xf[h, c] = new
                        xb[h, j] = new.astype(jnp.bfloat16)
                        z_ag(h, j, xb, up).start()

                    @pl.when(last)
                    def _():
                        xf[h, c] = new
                        x_local(h, c, j).start()
                        remote(xf.at[h, c], x_out.at[h, j], zag_s.at[h, j], zag_r.at[h, j], up).start()

            on(zt - RL * d, HP, reduce)

            def spread(d=d, down=down, up=up, base=base):
                j = base + zt - 3 * RL - AL * (3 - d)

                def kind(buf):
                    z_ag(h, j, buf, up).wait_recv()

                    @pl.when(d > 0)
                    def _():
                        z_ag(h, j, buf, up).start()

                z_rs(h, j, down).wait_send()
                by_kind(last, xb, x_out, kind)

            @pl.when(d < 3)
            def _(spread=spread, d=d):
                on(zt - 3 * RL - AL * (3 - d), HP, spread)

            def sent(d=d, up=up, base=base):
                c = zt - 3 * RL - AL * (4 - d)
                j = base + c

                def kind(buf):
                    z_ag(h, j, buf, up).wait_send()

                by_kind(last, xb, x_out, kind)

                @pl.when(jnp.logical_and(last, d == 3))
                def _():
                    x_local(h, c, j).wait()

            @pl.when(d > 0)
            def _(sent=sent, d=d):
                on(zt - 3 * RL - AL * (4 - d), HP, sent)

    def slot(t, _):
        state = []
        for h in (0, 1):
            u = t - h * OFFSET
            k = u // PERIOD
            v = u - k * PERIOD
            active = jnp.logical_and(u >= 0, k < SWEEPS)
            v = jnp.where(active, v, -1000)
            k = jnp.clip(k, 0, SWEEPS - 1)
            state.append((h, k, v, k == SWEEPS - 1))
        for h, k, v, last in state:
            @pl.when(jnp.logical_and(v >= 0, v < FSLOTS))
            def _(h=h, v=v):
                step1(h, v)
        for h, k, v, last in state:
            @pl.when(v >= FSLOTS)
            def _(h=h, v=v, last=last):
                z_steps(h, v, last)
        for h, k, v, last in state:
            @pl.when(jnp.logical_and(v >= 0, v < FSLOTS))
            def _(h=h, k=k, v=v, last=last):
                forward(h, k, v)
                step2(h, k, v, last)
                step3(h, v, last)
                backward(h, v, last)
        return 0

    lax.fori_loop(0, TOTAL, slot, 0)


def solution(mesh):
    ray_size = mesh.shape["ray"]

    def local_sweeps(a_blk, x_loc, sino_loc, row_inv, col_inv, relaxation):
        rays, pixels = a_blk.shape
        cols = x_loc.shape[1]
        rows, lanes = rays // NR, pixels // NP
        pix = lax.axis_index("pix")
        q = lax.rem(pix, 2) * 2 + pix // 2
        x0 = x_loc.reshape(NP, lanes, 2, 128).transpose(2, 0, 3, 1)
        own = lax.dynamic_slice_in_dim(sino_loc.reshape(NR, rows, 2, 4, 32), q, 1, axis=3)
        sino = own.reshape(NR, rows, 2, 32).transpose(2, 0, 3, 1)
        rinv = row_inv.reshape(NR, 1, rows)
        lamcol = (relaxation * col_inv).reshape(NP, 1, lanes)
        f32, bf16 = jnp.float32, jnp.bfloat16
        dma = pltpu.SemaphoreType.DMA
        anyspace = pl.BlockSpec(memory_space=pl.ANY)
        vmem = pl.BlockSpec(memory_space=pltpu.VMEM)
        x_new, r_new, sq = pl.pallas_call(
            sweep_kernel,
            out_shape=(
                jax.ShapeDtypeStruct((2, NP, 128, lanes), f32),
                jax.ShapeDtypeStruct((2, NR, 128, rows), f32),
                jax.ShapeDtypeStruct((SWEEPS, 64, 128), f32),
            ),
            in_specs=[anyspace, anyspace, anyspace, vmem, vmem, vmem],
            out_specs=(anyspace, anyspace, vmem),
            scratch_shapes=[
                pltpu.VMEM((rays, pixels), bf16),
                pltpu.VMEM((NR, 128, rows), f32),
                pltpu.VMEM((NR, 64, rows), f32),
                pltpu.VMEM((NR, 32, rows), f32),
                pltpu.VMEM((NR, 128, rows), bf16),
                pltpu.VMEM((2, NP, 128, lanes), f32),
                pltpu.VMEM((NP, 128, lanes), f32),
                pltpu.VMEM((2, HP, 128, lanes), f32),
                pltpu.VMEM((2, NP, 128, lanes), bf16),
                dma((NR,)), dma((2,)),
                dma((NR,)), dma((NR,)), dma((NR,)), dma((NR,)), dma((NR,)), dma((NR,)),
                dma((2, NR)), dma((2, NR)),
                dma((2, NP)), dma((2, NP)), dma((2, NP)), dma((2, NP)),
                dma((NR,)), dma((NR,)), dma((2, NR)), dma((2, NR)),
                dma((NR,)), dma((2, HP)),
            ],
            compiler_params=pltpu.CompilerParams(
                collective_id=0, has_side_effects=True, vmem_limit_bytes=67043328),
        )(a_blk, x0.astype(bf16), x0, sino, rinv, lamcol)
        x_fin = x_new.transpose(1, 3, 0, 2).reshape(pixels, cols)
        resid = r_new.transpose(1, 3, 0, 2).reshape(rays, cols)
        sums = jnp.sum(sq, axis=-1).reshape(SWEEPS, 2, 1, 32)
        spread = jnp.where(jnp.arange(4)[None, None, :, None] == q, sums, 0.0).reshape(SWEEPS, cols)
        sq_norms = lax.psum(spread, ("ray", "pix")) / (rays * ray_size)
        return x_fin, resid, sq_norms

    return jax.shard_map(
        local_sweeps,
        mesh=mesh,
        in_specs=(P("ray", "pix"), P("pix", "part"), P("ray", "part"), P("ray"), P("pix"), P()),
        out_specs=(P("pix", "part"), P("ray", "part"), P(None, "part")),
        check_vma=False,
    )
```
